32 devices in a mesh: depth: 2 (over x), row: 4 (over y, core), col: 4 (over z).
Axes of the slice: x: 2, y: 2, z: 4, core: 2. Of those that a mesh axis runs over, the one named last changes fastest.
Arguments:
- q_slab: float32 [1536, 1024], P('col', ('depth', 'row')), may hold values from -6 to 6
- triangle: float32 [1024, 1024], P(None, 'depth'), as said below
- panel_q: float32 [32768, 1024], P('row', ('depth', 'col')), may hold values from -0.1875 to 0.1875
Outputs:
- slab_out: float32 [1536, 32768], P('col', 'row')
The draws below stay inside these ranges and needn't reach their ends.
Inputs may be any that keep to these rules, and one draw needn't show every extreme that they name: triangle is zero below its diagonal; its diagonal lies in 0.5 to 1.5.
All inputs are finite; a program needn't handle non-finite values.
Results may differ from the reference program's by a relative error of at most 0.000071.
Values sent between devices are 32-bit elements; how exact they have to be, the bound alone decides.
A program may use at most 64 MiB of HBM per device.

```python
import math
import jax
import jax.numpy as jnp
from jax import lax

ORDER = 32768
K = 1024
SLAB = 1536


def draw_triangle(key, part):
    first, second = jax.random.split(jax.random.fold_in(key, 7))
    upper = jnp.clip(jax.random.normal(first, (K, K), jnp.float32), -4.0, 4.0)
    upper = upper / math.sqrt(K)
    diagonal = jax.random.uniform(second, (K,), jnp.float32, 0.5, 1.5)
    return jnp.triu(upper, 1) + jnp.diag(diagonal)


def block_levels(rng, shape, shards, low, largest):
    def one(dim, shards_of):
        heights = jax.random.uniform(jax.random.fold_in(jax.random.fold_in(rng, 6), dim), (shards_of,), jnp.float32, low / len(shards), largest / len(shards))
        return jnp.repeat(jnp.exp(heights), shape[dim] // shards_of).reshape((-1,) + (1,) * (len(shape) - dim - 1))

    gain = one(*shards[0])
    for cut in shards[1:]:
        gain = gain * one(*cut)
    return gain


def gaussian(key, shape, deviation, most, cuts=(), dtype=jnp.bfloat16):
    array = deviation * jax.random.normal(key, shape, jnp.float32)
    if cuts:
        array = array * block_levels(key, shape, cuts, -0.22, 0.18)
    return jnp.clip(array, -most, most).astype(dtype)


def setup_inputs(seed: int = 0) -> dict:
    seeds = jax.random.split(jax.random.key(seed), 4)
    q_slab = gaussian(seeds[0], (SLAB, K), 1.0, 6.0, ((0, 4), (1, 8)), jnp.float32)
    triangle = draw_triangle(jax.random.fold_in(seeds[3], 71), 0)
    panel_q = gaussian(seeds[2], (ORDER, K), K ** -0.5, 0.1875, ((0, 4), (1, 8)), jnp.float32)
    return {"q_slab": q_slab, "triangle": triangle, "panel_q": panel_q}


def reference(q_slab, triangle, panel_q):
    left = jnp.dot(q_slab, triangle, precision=lax.Precision.HIGHEST, preferred_element_type=jnp.float32)
    return lax.dot_general(left, panel_q, (((1,), (1,)), ((), ())), precision=lax.Precision.HIGHEST, preferred_element_type=jnp.float32)
```

```python
import functools

import jax
import jax.numpy as jnp
from jax import lax
from jax.experimental import pallas as pl
from jax.experimental.pallas import tpu as pltpu
from jax.sharding import PartitionSpec as P

MESH = pl.DeviceIdType.MESH
CHUNK = 256
AHEAD = 5


def split(x):
    high = x.astype(jnp.bfloat16)
    return high, (x - high.astype(jnp.float32)).astype(jnp.bfloat16)


def product(left, right):
    return lax.dot_general(
        left, right, (((1,), (1,)), ((), ())), preferred_element_type=jnp.float32
    )


def kernel(
    cols, half, panel, high_ref, low_ref, out, buf, made, part, got,
    own_sem, xs, xr, zs, zr, ps, pr, os, orr, ol,
):
    d, r, c = lax.axis_index("depth"), lax.axis_index("row"), lax.axis_index("col")
    steps = half // CHUNK
    slab = made.shape[1]
    last = cols - 1
    other = (1 - d, r, c)
    right = (d, r, (c + 1) % cols)
    left = (d, r, (c + cols - 1) % cols)

    def rows(start, k):
        return pl.ds(pl.multiple_of(start + k * CHUNK, CHUNK), CHUNK)

    def remote(src, dst, send, recv, to):
        return pltpu.make_async_remote_copy(
            src_ref=src, dst_ref=dst, send_sem=send, recv_sem=recv,
            device_id=to, device_id_type=MESH,
        )

    def swap(k, lane):
        return remote(
            panel.at[rows((1 - d) * half, k), :],
            buf.at[c, lane, rows(0, k), :],
            xs.at[k], xr.at[k], other,
        )

    def pass_on(way, b, k):
        ref = buf.at[b, :, rows(0, k), :]
        return remote(ref, ref, zs.at[way, b, k], zr.at[b, k], (right, left)[way])

    def send_part(way, k):
        return remote(part.at[k], got.at[k], ps.at[k], pr.at[k], (right, left)[way])

    def give(k, side):
        return remote(
            made.at[k], out.at[:, rows(side * half, k)], os.at[k], orr.at[k], other
        )

    def keep(k):
        return pltpu.make_async_copy(made.at[k], out.at[:, rows(d * half, k)], ol.at[k])

    own = pltpu.make_async_copy(
        panel.at[pl.ds(pl.multiple_of(d * half, half), half), :], buf.at[c, d], own_sem
    )
    own.start()

    @pl.loop(0, steps)
    def _(k):
        swap(k, d).start()

    own.wait()

    def forward(k):
        swap(k, 1 - d).wait_recv()

        @pl.when(c < last - 1)
        def _():
            pass_on(0, c, k).start()

        @pl.when(c > 1)
        def _():
            pass_on(1, c, k).start()

        for b in range(cols):

            @pl.when((b < c) & (c < last - 1))
            def _():
                pass_on(0, b, k).wait_recv()
                pass_on(0, b, k).start()

            @pl.when((b > c) & (c > 1))
            def _():
                pass_on(1, b, k).wait_recv()
                pass_on(1, b, k).start()

    def block(b, k):
        x = jnp.concatenate([buf[b, 0, rows(0, k), :], buf[b, 1, rows(0, k), :]], axis=1)
        return split(x)

    inner = (c >= 1) & (c <= last - 1)

    def compute(k):
        @pl.when(inner)
        def _():
            for b in range(cols):

                @pl.when(((b < c) & (c >= last - 1)) | ((b > c) & (c <= 1)))
                def _():
                    pass_on(0, b, k).wait_recv()

            total = None
            for b in range(cols):
                high, low = block(b, k)
                term = product(high_ref[b], high) + product(high_ref[b], low)
                term = term + product(low_ref[b], high)
                total = term if total is None else total + term
            made[k] = total[:slab]
            part[k] = total[slab:]

            @pl.when(c == 1)
            def _():
                send_part(1, k).start()

            @pl.when(c == last - 1)
            def _():
                send_part(0, k).start()

        @pl.when((c == 0) | (c == last))
        def _():
            high, low = block(c, k)
            left_high, left_low = high_ref[c, :slab], low_ref[c, :slab]
            total = product(left_high, high) + product(left_high, low)
            total = total + product(left_low, high)
            send_part(0, k).wait_recv()
            made[k] = total + got[k]

        give(k, d).start()
        keep(k).start()

    @pl.loop(0, min(AHEAD, steps))
    def _(k):
        forward(k)

    @pl.loop(0, steps)
    def _(k):
        @pl.when(k + AHEAD < steps)
        def _():
            forward(k + AHEAD)

        compute(k)

    @pl.loop(0, steps)
    def _(k):
        swap(k, d).wait_send()
        for b in range(cols):

            @pl.when((b <= c) & (c < last - 1))
            def _():
                pass_on(0, b, k).wait_send()

            @pl.when((b >= c) & (c > 1))
            def _():
                pass_on(1, b, k).wait_send()

        @pl.when((c == 1) | (c == last - 1))
        def _():
            send_part(0, k).wait_send()

        keep(k).wait()
        give(k, d).wait_send()
        give(k, 1 - d).wait_recv()


def lefts(q_slab, triangle):
    width = triangle.shape[1]
    share = width // lax.axis_size("row")
    factor = lax.dynamic_slice_in_dim(triangle, lax.axis_index("row") * share, share, 1)
    return jnp.dot(
        lax.all_gather(q_slab, ("depth", "row"), axis=1, tiled=True),
        factor,
        precision=lax.Precision.HIGHEST,
        preferred_element_type=jnp.float32,
    )


def lined(q_slab, triangle, panel_q):
    slab = q_slab.shape[0]
    total_rows, narrow = panel_q.shape
    half = total_rows // 2
    steps = half // CHUNK
    cols = lax.axis_size("col")
    c = lax.axis_index("col")
    share = lefts(q_slab, triangle)
    beside = lax.ppermute(share, "col", [(0, 1), (cols - 1, cols - 2)])
    both = jnp.concatenate([share, beside], axis=0)
    both = lax.all_gather(both, ("depth", "row"), axis=1, tiled=True)
    grid = both.reshape(2, slab, 2, cols, narrow).transpose(3, 0, 1, 2, 4)
    at = jnp.arange(cols)
    end = jnp.where(c == 1, 0, cols - 1)
    mask = jnp.stack([jnp.ones_like(at, bool), at != end], axis=1)
    grid = jnp.where(mask[:, :, None, None, None], grid, 0.0)
    grid = grid.reshape(cols, 2 * slab, 2 * narrow)
    high = lax.reduce_precision(grid, 8, 7)
    low = (grid - high).astype(jnp.bfloat16)
    high = high.astype(jnp.bfloat16)
    dma = pltpu.SemaphoreType.DMA
    piece = pltpu.VMEM((steps, slab, CHUNK), jnp.float32)
    return pl.pallas_call(
        functools.partial(kernel, cols, half),
        out_shape=jax.ShapeDtypeStruct((slab, total_rows), jnp.float32),
        in_specs=[
            pl.BlockSpec(memory_space=pl.ANY),
            pl.BlockSpec(memory_space=pltpu.VMEM),
            pl.BlockSpec(memory_space=pltpu.VMEM),
        ],
        out_specs=pl.BlockSpec(memory_space=pl.ANY),
        scratch_shapes=[
            pltpu.VMEM((cols, 2, half, narrow), jnp.float32),
            piece, piece, piece,
            dma, dma((steps,)), dma((steps,)),
            dma((2, cols, steps)), dma((cols, steps)),
            dma((steps,)), dma((steps,)),
            dma((steps,)), dma((steps,)), dma((steps,)),
        ],
        compiler_params=pltpu.CompilerParams(
            has_side_effects=True, vmem_limit_bytes=60 * 1024 * 1024
        ),
        name="back_transform",
    )(panel_q, high, low)


def gathered(q_slab, triangle, panel_q):
    rows = q_slab.shape[0]
    left = lax.all_gather(lefts(q_slab, triangle), "row", axis=1, tiled=True)
    narrow = panel_q.shape[1]
    columns = lax.axis_size("col")
    mixed = lax.all_to_all(panel_q, "depth", split_axis=0, concat_axis=1, tiled=True)
    left_all = lax.all_gather(left, "depth", axis=1, tiled=True)
    grid = left_all.reshape(rows, 2, columns, narrow)
    piece = lax.all_gather(mixed, "col", axis=1, tiled=True)
    count = piece.shape[1] // (2 * narrow)
    pieces = piece.reshape(piece.shape[0], count, 2, narrow)
    partial_out = jnp.einsum(
        "sdnw,rndw->sr",
        grid,
        pieces,
        precision=lax.Precision.HIGHEST,
        preferred_element_type=jnp.float32,
    )
    return lax.all_gather(partial_out, "depth", axis=1, tiled=True)


def per_device(q_slab, triangle, panel_q):
    rows, narrow = panel_q.shape
    held = 4 * rows * (narrow * lax.axis_size("col") + 2 * q_slab.shape[0])
    fits = held <= 48 * 1024 * 1024
    if narrow % 128 == 0 and rows % (2 * CHUNK) == 0 and lax.axis_size("col") >= 4 and fits:
        return lined(q_slab, triangle, panel_q)
    return gathered(q_slab, triangle, panel_q)


def solution(mesh):
    placed = (P("col", ("depth", "row")), P(None, "depth"), P("row", ("depth", "col")))
    return jax.shard_map(
        per_device, mesh=mesh, in_specs=placed, out_specs=P("col", "row"), check_vma=False
    )
```

```python
import functools

import jax
import jax.numpy as jnp
from jax import lax
from jax.experimental import pallas as pl
from jax.experimental.pallas import tpu as pltpu
from jax.sharding import PartitionSpec as P

MESH = pl.DeviceIdType.MESH
CHUNK = 256
AHEAD = 5
FIRST = 10


def split(x):
    high = x.astype(jnp.bfloat16)
    return high, (x - high.astype(jnp.float32)).astype(jnp.bfloat16)


def product(left, right):
    return lax.dot_general(
        left, right, (((1,), (1,)), ((), ())), preferred_element_type=jnp.float32
    )


def kernel(
    cols, half, slab_ref, factor_ref, panel, out, buf, made, part, got,
    q_buf, t_buf, l_buf, high_ref, low_ref,
    own_sem, xs, xr, zs, zr, ps, pr, os, orr, ol, mine, qs, qr, ls, lr, ns, nr,
):
    d, r, c = lax.axis_index("depth"), lax.axis_index("row"), lax.axis_index("col")
    steps = half // CHUNK
    slab = made.shape[1]
    last = cols - 1
    other = (1 - d, r, c)
    right = (d, r, (c + 1) % cols)
    left = (d, r, (c + cols - 1) % cols)

    def rows(start, k):
        return pl.ds(pl.multiple_of(start + k * CHUNK, CHUNK), CHUNK)

    def remote(src, dst, send, recv, to):
        return pltpu.make_async_remote_copy(
            src_ref=src, dst_ref=dst, send_sem=send, recv_sem=recv,
            device_id=to, device_id_type=MESH,
        )

    def swap(k, lane):
        return remote(
            panel.at[rows((1 - d) * half, k), :],
            buf.at[c, lane, rows(0, k), :],
            xs.at[k], xr.at[k], other,
        )

    def pass_on(way, b, k):
        ref = buf.at[b, :, rows(0, k), :]
        return remote(ref, ref, zs.at[way, b, k], zr.at[b, k], (right, left)[way])

    def send_part(way, k):
        return remote(part.at[k], got.at[k], ps.at[k], pr.at[k], (right, left)[way])

    def give(k, side):
        return remote(
            made.at[k], out.at[:, rows(side * half, k)], os.at[k], orr.at[k], other
        )

    def keep(k):
        return pltpu.make_async_copy(made.at[k], out.at[:, rows(d * half, k)], ol.at[k])

    def flip(at, bit):
        return at + bit * (1 - 2 * ((at // bit) % 2))

    me = d * cols + r

    def doubling(ref, send, recv):
        stages = [[remote(ref.at[me], ref.at[me], send.at[0], recv.at[0], other)]]
        held = [r]
        count = 1
        bit = cols // 2
        while bit:
            stage = []
            for side in (d, 1 - d):
                for at in held:
                    ours = ref.at[side * cols + at]
                    stage.append(
                        remote(ours, ours, send.at[count], recv.at[count], (d, flip(r, bit), c))
                    )
                    count += 1
            stages.append(stage)
            held = held + [flip(at, bit) for at in held]
            bit //= 2
        return stages

    def start(stage):
        for copy in stage:
            copy.start()

    def arrive(stage):
        for copy in stage:
            copy.wait_recv()

    own = pltpu.make_async_copy(
        panel.at[pl.ds(pl.multiple_of(d * half, half), half), :], buf.at[c, d], own_sem
    )
    share = t_buf.shape[1]
    loads = [
        pltpu.make_async_copy(slab_ref, q_buf.at[me], mine.at[0]),
        pltpu.make_async_copy(
            factor_ref.at[:, pl.ds(pl.multiple_of(r * share, share), share)], t_buf, mine.at[1]
        ),
    ]
    loads[0].start()
    own.start()
    loads[1].start()
    q_stages = doubling(q_buf, qs, qr)
    l_stages = doubling(l_buf, ls, lr)
    first = min(FIRST, steps)
    loads[0].wait()
    start(q_stages[0])

    @pl.loop(0, first)
    def _(k):
        swap(k, d).start()

    own.wait()

    def forward(k):
        swap(k, 1 - d).wait_recv()

        @pl.when(c < last - 1)
        def _():
            pass_on(0, c, k).start()

        @pl.when(c > 1)
        def _():
            pass_on(1, c, k).start()

        for b in range(cols):

            @pl.when((b < c) & (c < last - 1))
            def _():
                pass_on(0, b, k).wait_recv()
                pass_on(0, b, k).start()

            @pl.when((b > c) & (c > 1))
            def _():
                pass_on(1, b, k).wait_recv()
                pass_on(1, b, k).start()

    def block(b, k):
        x = jnp.concatenate([buf[b, 0, rows(0, k), :], buf[b, 1, rows(0, k), :]], axis=1)
        return split(x)

    inner = (c >= 1) & (c <= last - 1)

    def compute(k):
        @pl.when(inner)
        def _():
            for b in range(cols):

                @pl.when(((b < c) & (c >= last - 1)) | ((b > c) & (c <= 1)))
                def _():
                    pass_on(0, b, k).wait_recv()

            total = None
            for b in range(cols):
                high, low = block(b, k)
                term = product(high_ref[b], high) + product(high_ref[b], low)
                term = term + product(low_ref[b], high)
                total = term if total is None else total + term
            made[k] = total[:slab]
            part[k] = total[slab:]

            @pl.when(c == 1)
            def _():
                send_part(1, k).start()

            @pl.when(c == last - 1)
            def _():
                send_part(0, k).start()

        @pl.when((c == 0) | (c == last))
        def _():
            high, low = block(c, k)
            left_high, left_low = high_ref[c, :slab], low_ref[c, :slab]
            total = product(left_high, high) + product(left_high, low)
            total = total + product(left_low, high)
            send_part(0, k).wait_recv()
            made[k] = total + got[k]

        give(k, d).start()
        keep(k).start()

    arrive(q_stages[0])
    start(q_stages[1])
    forward(0)
    for before, after in zip(q_stages[1:], q_stages[2:] + [[]]):
        arrive(before)
        start(after)
    loads[1].wait()
    width = q_buf.shape[2]
    total = None
    for i in range(q_buf.shape[0]):
        q_high, q_low = split(q_buf[i])
        t_high, t_low = split(t_buf[i * width : (i + 1) * width, :])
        term = jnp.dot(q_high, t_high, preferred_element_type=jnp.float32)
        term = term + jnp.dot(q_high, t_low, preferred_element_type=jnp.float32)
        term = term + jnp.dot(q_low, t_high, preferred_element_type=jnp.float32)
        total = term if total is None else total + term
    l_buf[me, :slab, :] = total

    def beside(to):
        return remote(
            l_buf.at[me, :slab, :], l_buf.at[me, slab:, :], ns, nr, to
        )

    ends = (c == 0) | (c == last)
    helps = (c == 1) | (c == last - 1)

    @pl.when(c == 0)
    def _():
        beside(right).start()

    @pl.when(c == last)
    def _():
        beside(left).start()

    @pl.when((c != 1) & (c != last - 1))
    def _():
        l_buf[me, slab:, :] = jnp.zeros((slab, share), jnp.float32)

    forward(1)

    @pl.when(helps)
    def _():
        beside(left).wait_recv()

    start(l_stages[0])

    @pl.loop(first, steps)
    def _(k):
        swap(k, d).start()

    forward(2)
    for at, (before, after) in enumerate(zip(l_stages, l_stages[1:] + [[]])):
        arrive(before)
        start(after)
        if at == 0:
            forward(3)
    for b in range(cols):
        x = jnp.concatenate([l_buf[b], l_buf[cols + b]], axis=1)
        high, low = split(x)
        high_ref[b] = high
        low_ref[b] = low

    @pl.when(c == 1)
    def _():
        high_ref[0, slab:, :] = jnp.zeros((slab, 2 * share), jnp.bfloat16)
        low_ref[0, slab:, :] = jnp.zeros((slab, 2 * share), jnp.bfloat16)

    @pl.when(c == last - 1)
    def _():
        high_ref[last, slab:, :] = jnp.zeros((slab, 2 * share), jnp.bfloat16)
        low_ref[last, slab:, :] = jnp.zeros((slab, 2 * share), jnp.bfloat16)

    @pl.loop(4, AHEAD)
    def _(k):
        forward(k)

    @pl.loop(0, steps)
    def _(k):
        @pl.when(k + AHEAD < steps)
        def _():
            forward(k + AHEAD)

        compute(k)

    @pl.loop(0, steps)
    def _(k):
        swap(k, d).wait_send()
        for b in range(cols):

            @pl.when((b <= c) & (c < last - 1))
            def _():
                pass_on(0, b, k).wait_send()

            @pl.when((b >= c) & (c > 1))
            def _():
                pass_on(1, b, k).wait_send()

        @pl.when((c == 1) | (c == last - 1))
        def _():
            send_part(0, k).wait_send()

        keep(k).wait()
        give(k, d).wait_send()
        give(k, 1 - d).wait_recv()

    for stage in q_stages + l_stages:
        for copy in stage:
            copy.wait_send()

    @pl.when(ends)
    def _():
        beside(right).wait_send()


def lefts(q_slab, triangle):
    width = triangle.shape[1]
    share = width // lax.axis_size("row")
    factor = lax.dynamic_slice_in_dim(triangle, lax.axis_index("row") * share, share, 1)
    return jnp.dot(
        lax.all_gather(q_slab, ("depth", "row"), axis=1, tiled=True),
        factor,
        precision=lax.Precision.HIGHEST,
        preferred_element_type=jnp.float32,
    )


def lined(q_slab, triangle, panel_q):
    slab = q_slab.shape[0]
    total_rows, narrow = panel_q.shape
    half = total_rows // 2
    steps = half // CHUNK
    cols = lax.axis_size("col")
    dma = pltpu.SemaphoreType.DMA
    piece = pltpu.VMEM((steps, slab, CHUNK), jnp.float32)
    factor = pltpu.VMEM((cols, 2 * slab, 2 * narrow), jnp.bfloat16)
    return pl.pallas_call(
        functools.partial(kernel, cols, half),
        out_shape=jax.ShapeDtypeStruct((slab, total_rows), jnp.float32),
        in_specs=[
            pl.BlockSpec(memory_space=pl.ANY),
            pl.BlockSpec(memory_space=pl.ANY),
            pl.BlockSpec(memory_space=pl.ANY),
        ],
        out_specs=pl.BlockSpec(memory_space=pl.ANY),
        scratch_shapes=[
            pltpu.VMEM((cols, 2, half, narrow), jnp.float32),
            piece, piece, piece,
            pltpu.VMEM((2 * cols, slab, narrow), jnp.float32),
            pltpu.VMEM((2 * cols * narrow, narrow), jnp.float32),
            pltpu.VMEM((2 * cols, 2 * slab, narrow), jnp.float32),
            factor, factor,
            dma, dma((steps,)), dma((steps,)),
            dma((2, cols, steps)), dma((cols, steps)),
            dma((steps,)), dma((steps,)),
            dma((steps,)), dma((steps,)), dma((steps,)),
            dma((2,)),
            dma((2 * cols - 1,)), dma((2 * cols - 1,)),
            dma((2 * cols - 1,)), dma((2 * cols - 1,)),
            dma, dma,
        ],
        compiler_params=pltpu.CompilerParams(
            has_side_effects=True, vmem_limit_bytes=60 * 1024 * 1024
        ),
        name="back_transform",
    )(q_slab, triangle, panel_q)


def gathered(q_slab, triangle, panel_q):
    rows = q_slab.shape[0]
    left = lax.all_gather(lefts(q_slab, triangle), "row", axis=1, tiled=True)
    narrow = panel_q.shape[1]
    columns = lax.axis_size("col")
    mixed = lax.all_to_all(panel_q, "depth", split_axis=0, concat_axis=1, tiled=True)
    left_all = lax.all_gather(left, "depth", axis=1, tiled=True)
    grid = left_all.reshape(rows, 2, columns, narrow)
    piece = lax.all_gather(mixed, "col", axis=1, tiled=True)
    count = piece.shape[1] // (2 * narrow)
    pieces = piece.reshape(piece.shape[0], count, 2, narrow)
    partial_out = jnp.einsum(
        "sdnw,rndw->sr",
        grid,
        pieces,
        precision=lax.Precision.HIGHEST,
        preferred_element_type=jnp.float32,
    )
    return lax.all_gather(partial_out, "depth", axis=1, tiled=True)


def per_device(q_slab, triangle, panel_q):
    rows, narrow = panel_q.shape
    held = 4 * rows * (narrow * lax.axis_size("col") + 2 * q_slab.shape[0])
    fits = held <= 48 * 1024 * 1024
    cols = lax.axis_size("col")
    even = cols >= 4 and cols & (cols - 1) == 0 and lax.axis_size("row") == cols
    deep = rows % (2 * CHUNK) == 0 and rows >= 2 * CHUNK * AHEAD
    if even and deep and narrow % 128 == 0 and fits:
        return lined(q_slab, triangle, panel_q)
    return gathered(q_slab, triangle, panel_q)


def solution(mesh):
    placed = (P("col", ("depth", "row")), P(None, "depth"), P("row", ("depth", "col")))
    return jax.shard_map(
        per_device, mesh=mesh, in_specs=placed, out_specs=P("col", "row"), check_vma=False
    )
```

```python
import functools

import jax
import jax.numpy as jnp
from jax import lax
from jax.experimental import pallas as pl
from jax.experimental.pallas import tpu as pltpu
from jax.sharding import PartitionSpec as P

MESH = pl.DeviceIdType.MESH
CHUNK = 512
AHEAD = 4
FIRST = 3


def split(x):
    high = x.astype(jnp.bfloat16)
    return high, (x - high.astype(jnp.float32)).astype(jnp.bfloat16)


def product(left, right):
    return lax.dot_general(
        left, right, (((1,), (1,)), ((), ())), preferred_element_type=jnp.float32
    )


def kernel(
    cols, half, slab_ref, factor_ref, panel, out, buf, made, part, got,
    q_buf, t_buf, l_buf, high_ref, low_ref,
    own_sem, xs, xr, zs, zr, ps, pr, os, orr, ol, mine, qs, qr, ls, lr, ns, nr,
):
    d, r, c = lax.axis_index("depth"), lax.axis_index("row"), lax.axis_index("col")
    steps = half // CHUNK
    slab = made.shape[1]
    last = cols - 1
    other = (1 - d, r, c)
    right = (d, r, (c + 1) % cols)
    left = (d, r, (c + cols - 1) % cols)

    def rows(start, k):
        return pl.ds(pl.multiple_of(start + k * CHUNK, CHUNK), CHUNK)

    def remote(src, dst, send, recv, to):
        return pltpu.make_async_remote_copy(
            src_ref=src, dst_ref=dst, send_sem=send, recv_sem=recv,
            device_id=to, device_id_type=MESH,
        )

    def swap(k, lane):
        return remote(
            panel.at[rows((1 - d) * half, k), :],
            buf.at[c, lane, rows(0, k), :],
            xs.at[k], xr.at[k], other,
        )

    def pass_on(way, at, k):
        ref = buf.at[slice(0, at + 1) if way == 0 else slice(at, cols), :, rows(0, k), :]
        return remote(ref, ref, zs.at[way, k], zr.at[way, k], (right, left)[way])

    def send_part(way, k):
        return remote(part.at[k], got.at[k], ps.at[k], pr.at[k], (right, left)[way])

    def give(k, side):
        return remote(
            made.at[k], out.at[:, rows(side * half, k)], os.at[k], orr.at[k], other
        )

    def keep(k):
        return pltpu.make_async_copy(made.at[k], out.at[:, rows(d * half, k)], ol.at[k])

    def flip(at, bit):
        return at + bit * (1 - 2 * ((at // bit) % 2))

    me = d * cols + r

    def doubling(ref, send, recv):
        stages = [[remote(ref.at[me], ref.at[me], send.at[0], recv.at[0], other)]]
        held = [r]
        count = 1
        bit = cols // 2
        while bit:
            stage = []
            for side in (d, 1 - d):
                for at in held:
                    ours = ref.at[side * cols + at]
                    stage.append(
                        remote(ours, ours, send.at[count], recv.at[count], (d, flip(r, bit), c))
                    )
                    count += 1
            stages.append(stage)
            held = held + [flip(at, bit) for at in held]
            bit //= 2
        return stages

    def start(stage):
        for copy in stage:
            copy.start()

    def arrive(stage):
        for copy in stage:
            copy.wait_recv()

    own = pltpu.make_async_copy(
        panel.at[pl.ds(pl.multiple_of(d * half, half), half), :], buf.at[c, d], own_sem
    )
    share = t_buf.shape[1]
    loads = [
        pltpu.make_async_copy(slab_ref, q_buf.at[me], mine.at[0]),
        pltpu.make_async_copy(
            factor_ref.at[:, pl.ds(pl.multiple_of(r * share, share), share)], t_buf, mine.at[1]
        ),
    ]
    loads[0].start()
    own.start()
    loads[1].start()
    q_stages = doubling(q_buf, qs, qr)
    l_stages = doubling(l_buf, ls, lr)
    first = min(FIRST, steps)
    loads[0].wait()
    start(q_stages[0])

    @pl.loop(0, first)
    def _(k):
        swap(k, d).start()

    own.wait()

    def forward(k):
        swap(k, 1 - d).wait_recv()

        for at in range(cols):

            @pl.when(c == at)
            def _():
                if at < last - 1:
                    if at > 0:
                        pass_on(0, at - 1, k).wait_recv()
                    pass_on(0, at, k).start()
                if at > 1:
                    if at < last:
                        pass_on(1, at + 1, k).wait_recv()
                    pass_on(1, at, k).start()

    def block(b, k):
        x = jnp.concatenate([buf[b, 0, rows(0, k), :], buf[b, 1, rows(0, k), :]], axis=1)
        return split(x)

    inner = (c >= 1) & (c <= last - 1)

    def compute(k):
        @pl.when(inner)
        def _():
            @pl.when(c == last - 1)
            def _():
                pass_on(0, last - 2, k).wait_recv()

            @pl.when(c == 1)
            def _():
                pass_on(1, 2, k).wait_recv()

            total = None
            for b in range(cols):
                high, low = block(b, k)
                term = product(high_ref[b], high) + product(high_ref[b], low)
                term = term + product(low_ref[b], high)
                total = term if total is None else total + term
            made[k] = total[:slab]
            part[k] = total[slab:]

            @pl.when(c == 1)
            def _():
                send_part(1, k).start()

            @pl.when(c == last - 1)
            def _():
                send_part(0, k).start()

        @pl.when((c == 0) | (c == last))
        def _():
            high, low = block(c, k)
            left_high, left_low = high_ref[c, :slab], low_ref[c, :slab]
            total = product(left_high, high) + product(left_high, low)
            total = total + product(left_low, high)
            send_part(0, k).wait_recv()
            made[k] = total + got[k]

        give(k, d).start()
        keep(k).start()

    arrive(q_stages[0])
    start(q_stages[1])
    forward(0)
    for before, after in zip(q_stages[1:], q_stages[2:] + [[]]):
        arrive(before)
        start(after)
    loads[1].wait()
    width = q_buf.shape[2]
    total = None
    for i in range(q_buf.shape[0]):
        q_high, q_low = split(q_buf[i])
        t_high, t_low = split(t_buf[i * width : (i + 1) * width, :])
        term = jnp.dot(q_high, t_high, preferred_element_type=jnp.float32)
        term = term + jnp.dot(q_high, t_low, preferred_element_type=jnp.float32)
        term = term + jnp.dot(q_low, t_high, preferred_element_type=jnp.float32)
        total = term if total is None else total + term
    l_buf[me, :slab, :] = total

    def beside(to):
        return remote(
            l_buf.at[me, :slab, :], l_buf.at[me, slab:, :], ns, nr, to
        )

    ends = (c == 0) | (c == last)
    helps = (c == 1) | (c == last - 1)

    @pl.when(c == 0)
    def _():
        beside(right).start()

    @pl.when(c == last)
    def _():
        beside(left).start()

    @pl.when((c != 1) & (c != last - 1))
    def _():
        l_buf[me, slab:, :] = jnp.zeros((slab, share), jnp.float32)

    forward(1)

    @pl.when(helps)
    def _():
        beside(left).wait_recv()

    start(l_stages[0])

    @pl.loop(first, steps)
    def _(k):
        swap(k, d).start()

    for at, (before, after) in enumerate(zip(l_stages, l_stages[1:] + [[]])):
        arrive(before)
        start(after)
        if at == 0:
            forward(2)
            forward(3)
    for b in range(cols):
        x = jnp.concatenate([l_buf[b], l_buf[cols + b]], axis=1)
        high, low = split(x)
        high_ref[b] = high
        low_ref[b] = low

    @pl.when(c == 1)
    def _():
        high_ref[0, slab:, :] = jnp.zeros((slab, 2 * share), jnp.bfloat16)
        low_ref[0, slab:, :] = jnp.zeros((slab, 2 * share), jnp.bfloat16)

    @pl.when(c == last - 1)
    def _():
        high_ref[last, slab:, :] = jnp.zeros((slab, 2 * share), jnp.bfloat16)
        low_ref[last, slab:, :] = jnp.zeros((slab, 2 * share), jnp.bfloat16)

    @pl.loop(4, AHEAD)
    def _(k):
        forward(k)

    @pl.loop(0, steps)
    def _(k):
        @pl.when(k + AHEAD < steps)
        def _():
            forward(k + AHEAD)

        compute(k)

    @pl.loop(0, steps)
    def _(k):
        swap(k, d).wait_send()
        for at in range(cols):

            @pl.when(c == at)
            def _():
                if at < last - 1:
                    pass_on(0, at, k).wait_send()
                if at > 1:
                    pass_on(1, at, k).wait_send()

        @pl.when((c == 1) | (c == last - 1))
        def _():
            send_part(0, k).wait_send()

        keep(k).wait()
        give(k, d).wait_send()
        give(k, 1 - d).wait_recv()

    for stage in q_stages + l_stages:
        for copy in stage:
            copy.wait_send()

    @pl.when(ends)
    def _():
        beside(right).wait_send()


def lefts(q_slab, triangle):
    width = triangle.shape[1]
    share = width // lax.axis_size("row")
    factor = lax.dynamic_slice_in_dim(triangle, lax.axis_index("row") * share, share, 1)
    return jnp.dot(
        lax.all_gather(q_slab, ("depth", "row"), axis=1, tiled=True),
        factor,
        precision=lax.Precision.HIGHEST,
        preferred_element_type=jnp.float32,
    )


def lined(q_slab, triangle, panel_q):
    slab = q_slab.shape[0]
    total_rows, narrow = panel_q.shape
    half = total_rows // 2
    steps = half // CHUNK
    cols = lax.axis_size("col")
    dma = pltpu.SemaphoreType.DMA
    piece = pltpu.VMEM((steps, slab, CHUNK), jnp.float32)
    factor = pltpu.VMEM((cols, 2 * slab, 2 * narrow), jnp.bfloat16)
    return pl.pallas_call(
        functools.partial(kernel, cols, half),
        out_shape=jax.ShapeDtypeStruct((slab, total_rows), jnp.float32),
        in_specs=[
            pl.BlockSpec(memory_space=pl.ANY),
            pl.BlockSpec(memory_space=pl.ANY),
            pl.BlockSpec(memory_space=pl.ANY),
        ],
        out_specs=pl.BlockSpec(memory_space=pl.ANY),
        scratch_shapes=[
            pltpu.VMEM((cols, 2, half, narrow), jnp.float32),
            piece, piece, piece,
            pltpu.VMEM((2 * cols, slab, narrow), jnp.float32),
            pltpu.VMEM((2 * cols * narrow, narrow), jnp.float32),
            pltpu.VMEM((2 * cols, 2 * slab, narrow), jnp.float32),
            factor, factor,
            dma, dma((steps,)), dma((steps,)),
            dma((2, steps)), dma((2, steps)),
            dma((steps,)), dma((steps,)),
            dma((steps,)), dma((steps,)), dma((steps,)),
            dma((2,)),
            dma((2 * cols - 1,)), dma((2 * cols - 1,)),
            dma((2 * cols - 1,)), dma((2 * cols - 1,)),
            dma, dma,
        ],
        compiler_params=pltpu.CompilerParams(
            has_side_effects=True, vmem_limit_bytes=60 * 1024 * 1024
        ),
        name="back_transform",
    )(q_slab, triangle, panel_q)


def gathered(q_slab, triangle, panel_q):
    rows = q_slab.shape[0]
    left = lax.all_gather(lefts(q_slab, triangle), "row", axis=1, tiled=True)
    narrow = panel_q.shape[1]
    columns = lax.axis_size("col")
    mixed = lax.all_to_all(panel_q, "depth", split_axis=0, concat_axis=1, tiled=True)
    left_all = lax.all_gather(left, "depth", axis=1, tiled=True)
    grid = left_all.reshape(rows, 2, columns, narrow)
    piece = lax.all_gather(mixed, "col", axis=1, tiled=True)
    count = piece.shape[1] // (2 * narrow)
    pieces = piece.reshape(piece.shape[0], count, 2, narrow)
    partial_out = jnp.einsum(
        "sdnw,rndw->sr",
        grid,
        pieces,
        precision=lax.Precision.HIGHEST,
        preferred_element_type=jnp.float32,
    )
    return lax.all_gather(partial_out, "depth", axis=1, tiled=True)


def per_device(q_slab, triangle, panel_q):
    rows, narrow = panel_q.shape
    held = 4 * rows * (narrow * lax.axis_size("col") + 2 * q_slab.shape[0])
    fits = held <= 48 * 1024 * 1024
    cols = lax.axis_size("col")
    even = cols >= 4 and cols & (cols - 1) == 0 and lax.axis_size("row") == cols
    deep = rows % (2 * CHUNK) == 0 and rows >= 2 * CHUNK * AHEAD
    if even and deep and narrow % 128 == 0 and fits:
        return lined(q_slab, triangle, panel_q)
    return gathered(q_slab, triangle, panel_q)


def solution(mesh):
    placed = (P("col", ("depth", "row")), P(None, "depth"), P("row", ("depth", "col")))
    return jax.shard_map(
        per_device, mesh=mesh, in_specs=placed, out_specs=P("col", "row"), check_vma=False
    )
```
